128 devices in a mesh: row: 16 (over y, x), col: 4 (over z), depth: 2 (over core).
Axes of the slice: x: 4, y: 4, z: 4, core: 2. Of those that a mesh axis runs over, the one named last changes fastest.
Arguments:
- layers: float32 [2, 16384, 16384], P('depth', 'row', 'col'), may hold values from -3 to 265.4, as said below
Outputs:
- factor: float32 [2, 16384, 512], P(None, 'row', 'depth')
- schur: float32 [16384, 16384], P(('row', 'depth'), 'col')
The draws below stay inside these ranges and needn't reach their ends.
Inputs may be any that keep to these rules, and one draw needn't show every extreme that they name: Read in matrix order, each layer is symmetric, and the sum over layers is symmetric positive definite with a diagonal of order sqrt(16384).
All inputs are finite; a program needn't handle non-finite values.
Results may differ from the reference program's by a relative error of at most 0.0001.
Values sent between devices are 32-bit elements; how exact they have to be, the bound alone decides.
A program may use at most 192 MiB of HBM per device.

```python
import jax
import jax.numpy as jnp
from jax import lax

PANEL = 512
BLOCKS_DEV = 2
PANELS = 2
LAYERS = 2
ORDER = 16384
COL_BLOCKS = 8
N_ROW = 16
N_COL = 4


def draw_layers(key, part):
    row_groups = ORDER // (PANEL * BLOCKS_DEV)
    col_groups = ORDER // (PANEL * COL_BLOCKS)
    positions = jnp.arange(ORDER, dtype=jnp.float32)
    distance = jnp.abs(positions[:, None] - positions[None, :])

    def one_layer(layer_index):
        layer_key = jax.random.fold_in(key, layer_index)
        noise_key, diag_key, scale_key, amp_key, reach_key = jax.random.split(layer_key, 5)
        noise = jnp.clip(jax.random.normal(noise_key, (ORDER, ORDER), jnp.float32), -4.0, 4.0)
        reach = PANEL * jax.random.uniform(reach_key, (), jnp.float32, 0.04, 0.12)
        amplitude = ORDER ** 0.5 * jax.random.uniform(amp_key, (), jnp.float32, 0.2, 0.45)
        symmetric = (noise + noise.T) * (0.5 / 1.4142135)
        row_scale = jax.random.uniform(scale_key, (ORDER,), jnp.float32, 0.7, 1.3)
        kernel = amplitude * row_scale[:, None] * row_scale[None, :] * jnp.exp(-distance / reach)
        diag_values = ORDER ** 0.5 * jax.random.uniform(diag_key, (ORDER,), jnp.float32, 0.75, 1.25)
        matrix = symmetric + kernel + jnp.diag(diag_values)
        rows = matrix.reshape(BLOCKS_DEV, row_groups, PANEL, ORDER).transpose(1, 0, 2, 3).reshape(ORDER, ORDER)
        return rows.reshape(ORDER, COL_BLOCKS, col_groups, PANEL).transpose(0, 2, 1, 3).reshape(ORDER, ORDER)
    return lax.map(one_layer, jnp.arange(LAYERS, dtype=jnp.int32)).astype(jnp.float32)


def setup_inputs(seed: int = 0) -> dict:
    streams_of = jax.random.split(jax.random.key(seed), 2)
    layers = draw_layers(jax.random.fold_in(streams_of[1], 71), 0)
    return dict(layers=layers)


def to_matrix(array):
    rows = array.reshape(N_ROW, BLOCKS_DEV, PANEL, ORDER).transpose(1, 0, 2, 3).reshape(ORDER, ORDER)
    return rows.reshape(ORDER, N_COL, COL_BLOCKS, PANEL).transpose(0, 2, 1, 3).reshape(ORDER, ORDER)

def rows_to_storage(matrix):
    width = matrix.shape[1]
    return matrix.reshape(BLOCKS_DEV, N_ROW, PANEL, width).transpose(1, 0, 2, 3).reshape(ORDER, width)

def to_storage(matrix):
    rows = rows_to_storage(matrix)
    return rows.reshape(ORDER, COL_BLOCKS, N_COL, PANEL).transpose(0, 2, 1, 3).reshape(ORDER, ORDER)

def reference(layers):
    matrix = to_matrix(jnp.sum(layers, axis=0))
    identity_block = jnp.eye(PANEL, dtype=jnp.float32)
    columns = []
    for panel_step in range(PANELS):
        first = panel_step * PANEL
        after = first + PANEL
        lower_diag = jnp.linalg.cholesky(matrix[first:after, first:after])
        inverse = jax.scipy.linalg.solve_triangular(lower_diag, identity_block, lower=True)
        solved = jnp.dot(matrix[first:, first:after], inverse.T, precision=lax.Precision.HIGHEST)
        column = jnp.concatenate([jnp.zeros((first, PANEL), jnp.float32), solved], axis=0)
        columns.append(rows_to_storage(column))
        below = solved[PANEL:]
        update = jnp.dot(below, below.T, precision=lax.Precision.HIGHEST)
        matrix = matrix.at[after:, after:].add(-update)
    return (jnp.stack(columns), to_storage(matrix))
```

```python
import jax
import jax.numpy as jnp
from jax import lax
from jax.experimental import pallas as pl
from jax.experimental.pallas import tpu as pltpu
from jax.sharding import PartitionSpec as P

PANEL = 512
BLOCK = 128
HI = lax.Precision.HIGHEST
MESH = pl.DeviceIdType.MESH
F32 = jnp.float32


def inverse_factor(x):
    n = x.shape[0]
    lane8 = lax.broadcasted_iota(jnp.int32, (8, n), 1)
    sub8 = lax.broadcasted_iota(jnp.int32, (8, n), 0)
    out = []
    for k in range(n // 8):
        lo = 8 * k
        head, rest = x[:8], x[8:]
        ck = [jnp.broadcast_to(head[:, lo + j : lo + j + 1], (8, n)) for j in range(8)]
        inblk = (lane8 >= lo) & (lane8 < lo + 8)
        head = jnp.where(inblk, jnp.where(lane8 - lo == sub8, 1.0, 0.0), head)
        more = rest.shape[0] > 0
        if more:
            cr = [jnp.broadcast_to(rest[:, lo + j : lo + j + 1], rest.shape) for j in range(8)]
            lane = lax.broadcasted_iota(jnp.int32, rest.shape, 1)
            rest = jnp.where((lane >= lo) & (lane < lo + 8), 0.0, rest)
        pivots = ck[0]
        for j in range(8):
            if j:
                pivots = jnp.where(sub8 == j, ck[j], pivots)
            inv = 1.0 / ck[j][j : j + 1, :]
            mk = jnp.where(sub8 > j, ck[j], 0.0) * inv
            if more:
                mr = cr[j] * inv
            for t in range(j + 1, 8):
                row = ck[t][j : j + 1, :]
                ck[t] = ck[t] - mk * row
                if more:
                    cr[t] = cr[t] - mr * row
            row = head[j : j + 1, :]
            head = head - mk * row
            if more:
                rest = rest - mr * row
        out.append(jnp.where(lane8 <= sub8 + lo, head, 0.0) * lax.rsqrt(pivots))
        x = rest
    return jnp.concatenate(out, axis=0)


def factor_steps(v_ref, urow):
    size = v_ref.shape[0]
    blocks = size // BLOCK

    def step(j, carry):
        off = pl.multiple_of(j * BLOCK, BLOCK)
        here = pl.ds(off, BLOCK)
        w = inverse_factor(v_ref[here, here])
        urow[...] = jnp.dot(w, v_ref[here, :], precision=HI, preferred_element_type=F32)
        urow[:, here] = w
        for i in range(1, blocks):

            @pl.when(i > j)
            def _():
                rows = pl.ds(i * BLOCK, BLOCK)
                v_ref[rows, here] = jnp.zeros((BLOCK, BLOCK), F32)
                v_ref[rows, :] -= lax.dot_general(
                    urow[:, rows],
                    urow[...],
                    (((0,), (0,)), ((), ())),
                    precision=HI,
                    preferred_element_type=F32,
                )

        lane = lax.broadcasted_iota(jnp.int32, (BLOCK, size), 1)
        v_ref[here, :] = jnp.where(lane < off + BLOCK, urow[...], 0.0)
        return carry

    lax.fori_loop(0, blocks, step, 0)


def factor_kernel(d_ref, v_ref, urow):
    v_ref[:PANEL, :PANEL] = d_ref[0]
    v_ref[:PANEL, PANEL:] = d_ref[1]
    v_ref[PANEL:, :PANEL] = jnp.zeros((PANEL, PANEL), F32)
    v_ref[PANEL:, PANEL:] = d_ref[2]
    factor_steps(v_ref, urow)


def inverse_cholesky(d):
    size = 2 * PANEL
    return pl.pallas_call(
        factor_kernel,
        out_shape=jax.ShapeDtypeStruct((size, size), F32),
        in_specs=[pl.BlockSpec(memory_space=pltpu.VMEM)],
        out_specs=pl.BlockSpec(memory_space=pltpu.VMEM),
        scratch_shapes=[pltpu.VMEM((BLOCK, size), F32)],
        compiler_params=pltpu.CompilerParams(vmem_limit_bytes=32 * 2**20),
        name="factor",
    )(d)


ORDERS = ((2, 1, 0), (0, 2, 1), (1, 0, 2))
SOURCES = ((0, 0, 0), (0, 0, 1), (1, 0, 1))


def gather_kernel(layer, d_out, g_out, o_out, theirs, q, sem):
    (swap_s, swap_r, half_s, dsc_s, dsc_r, dph_s, dph_r, dsw_s, dsw_r,
     sc_s, sc_r, own_s, own_r, ag_s, ag_r) = sem
    r = lax.axis_index("row")
    z = lax.axis_index("col")
    d = lax.axis_index("depth")
    x = lax.rem(r, 4)
    y = lax.div(r, 4)
    here = (x, y, z)

    def device(c, depth):
        return (c[1] * 4 + c[0], c[2], depth)

    def remote(src, dst, send, recv, target):
        return pltpu.make_async_remote_copy(
            src_ref=src, dst_ref=dst, send_sem=send, recv_sem=recv, device_id=target, device_id_type=MESH
        )

    def moved(axis, by):
        c = list(here)
        c[axis] = lax.rem(c[axis] + by, 4)
        return tuple(c)

    mine = pl.ds(pl.multiple_of(d * PANEL, PANEL), PANEL)
    other = pl.ds(pl.multiple_of((1 - d) * PANEL, PANEL), PANEL)
    cols = pl.ds(0, PANEL)
    swap = remote(layer.at[other, cols], theirs, swap_s, swap_r, device(here, 1 - d))
    swap.start()
    local = pltpu.make_async_copy(layer.at[mine, cols], q, half_s)
    local.start()
    local.wait()
    swap.wait()
    q[...] = q[...] + theirs[...]

    half = PANEL // 2
    for b in range(3):
        sx, sy, sz = SOURCES[b]
        a1, a2, a3 = ORDERS[b]

        @pl.when((x == sx) & (y == sy) & (z == sz) & (d == 0))
        def _():
            def send(i, carry):
                c = [None] * 3
                piece = lax.div(i, 2)
                depth = lax.rem(i, 2)
                c[a1] = lax.rem(piece, 4)
                c[a2] = lax.rem(lax.div(piece, 4), 4)
                c[a3] = lax.div(piece, 16)
                rows = pl.ds(pl.multiple_of(piece * 8, 8), 8)
                part = pl.ds(pl.multiple_of(depth * half, half), half)
                own = (c[0] == sx) & (c[1] == sy) & (c[2] == sz) & (depth == 0)

                @pl.when(jnp.logical_not(own))
                def _():
                    remote(q.at[rows, part], d_out.at[b, rows, part], dsc_s.at[b], dsc_r.at[b], device(c, depth)).start()

                @pl.when(own)
                def _():
                    pltpu.make_async_copy(q.at[rows, part], d_out.at[b, rows, part], dsc_r.at[b]).start()

                return carry

            lax.fori_loop(0, 128, send, 0)

    for p in range(2):

        @pl.when(z == p)
        def _():
            for k in range(4):
                rows = pl.ds(k * BLOCK, BLOCK)
                target = g_out.at[y, k, :, pl.ds(p * PANEL, PANEL)]
                own = (x == p) & (x == k)

                @pl.when(jnp.logical_not(own))
                def _():
                    remote(q.at[rows, :], target, sc_s.at[k], sc_r.at[p], device((k, y, x), d)).start()

                @pl.when(own)
                def _():
                    pltpu.make_async_copy(q.at[rows, :], target, sc_r.at[p]).start()

    part = pl.ds(pl.multiple_of(d * half, half), half)

    def region(b, phase):
        a1, a2, a3 = ORDERS[b]
        c = here
        if phase == 0:
            return c[a3] * 128 + c[a2] * 32 + c[a1] * 8, 8
        if phase == 1:
            return c[a3] * 128 + c[a2] * 32, 32
        return c[a3] * 128, 128

    def phase_copy(b, phase, by):
        start, rows = region(b, phase)
        ref = d_out.at[b, pl.ds(pl.multiple_of(start, rows), rows), part]
        return remote(
            ref, ref, dph_s.at[b, phase, by - 1], dph_r.at[b, phase, by - 1], device(moved(ORDERS[b][phase], by), d)
        )

    def sized(ref, s):
        return pltpu.make_async_copy(ref, ref, s)

    for b in range(3):
        sized(d_out.at[b, pl.ds(0, 8), pl.ds(0, half)], dsc_r.at[b]).wait()
        for by in (1, 2, 3):
            phase_copy(b, 0, by).start()
    for phase in (1, 2):
        for b in range(3):
            for by in (1, 2, 3):
                phase_copy(b, phase - 1, by).wait_recv()
            for by in (1, 2, 3):
                phase_copy(b, phase, by).start()
    for b in range(3):
        for by in (1, 2, 3):
            phase_copy(b, 2, by).wait_recv()

        ref = d_out.at[b, :, part]
        remote(ref, ref, dsw_s.at[b], dsw_r.at[b], device(here, 1 - d)).start()

    def own_copy(p, to, slot):
        src = q
        return remote(src, o_out.at[p], own_s.at[slot], own_r.at[p], device((x, y, to), d))

    for p in range(2):

        @pl.when(z == p)
        def _():
            pltpu.make_async_copy(q, o_out.at[p], own_r.at[p]).start()
            own_copy(p, 1 - p, 0).start()
            own_copy(p, 3 - p, 1).start()

    for b in range(3):
        ref = d_out.at[b, :, part]
        remote(ref, ref, dsw_s.at[b], dsw_r.at[b], device(here, 1 - d)).wait()
        for phase in range(3):
            for by in (1, 2, 3):
                phase_copy(b, phase, by).wait_send()
        sx, sy, sz = SOURCES[b]

        @pl.when((x == sx) & (y == sy) & (z == sz) & (d == 0))
        def _():
            sized(layer.at[pl.ds(0, 127 * 8), pl.ds(0, half)], dsc_s.at[b]).wait()

    def ag_ref(h, phase, c, piece):
        cx, cy = c
        part = pl.ds(h * PANEL, PANEL)
        if phase == 0:
            rows = {None: pl.ds(0, 128), 0: pl.ds(0, 64), 1: pl.ds(64, 64)}[piece]
            return g_out.at[cy, cx, rows, part]
        span = {None: pl.ds(0, 4), 0: pl.ds(0, 2), 1: pl.ds(2, 2)}[piece]
        if h == 0:
            return g_out.at[cy, span, :, part]
        return g_out.at[span, cx, :, part]

    def ag_copy(h, phase, stage, way):
        axis = (phase + h) % 2
        by = 1 if way == 0 else 3
        c = here if stage == 0 else moved(axis, 4 - by)
        ref = ag_ref(h, phase, (c[0], c[1]), None if stage == 0 else way)
        slot = ((h * 2 + phase) * 2 + stage) * 2 + way
        return remote(ref, ref, ag_s.at[slot], ag_r.at[slot], device(moved(axis, by), d))

    for h in range(2):
        sized(g_out.at[0, 0, :, pl.ds(0, PANEL)], sc_r.at[h]).wait()
        for way in range(2):
            ag_copy(h, 0, 0, way).start()
    for phase in range(2):
        for h in range(2):
            for way in range(2):
                ag_copy(h, phase, 0, way).wait_recv()
            for way in range(2):
                ag_copy(h, phase, 1, way).start()
        for h in range(2):
            for way in range(2):
                ag_copy(h, phase, 1, way).wait_recv()
            if phase == 0:
                for way in range(2):
                    ag_copy(h, 1, 0, way).start()
        if phase == 0:
            for p in range(2):

                @pl.when(z == 3 - p)
                def _():
                    sized(o_out.at[p], own_r.at[p]).wait()
                    ref = o_out.at[p]
                    remote(ref, ref, own_s.at[0], own_r.at[p], device((x, y, 2 + p), d)).start()

    for p in range(2):

        @pl.when(z != 3 - p)
        def _():
            sized(o_out.at[p], own_r.at[p]).wait()

    for h in range(2):
        for phase in range(2):
            for stage in range(2):
                for way in range(2):
                    ag_copy(h, phase, stage, way).wait_send()

    @pl.when(z < 2)
    def _():
        sized(q, own_s.at[0]).wait()
        sized(q, own_s.at[1]).wait()

    @pl.when(z >= 2)
    def _():
        sized(q, own_s.at[0]).wait()

    for k in range(4):

        @pl.when((z < 2) & jnp.logical_not((x == z) & (x == k)))
        def _():
            sized(q.at[pl.ds(0, BLOCK), :], sc_s.at[k]).wait()


def gather_panels(layer):
    dma = pltpu.SemaphoreType.DMA
    return pl.pallas_call(
        gather_kernel,
        out_shape=[
            jax.ShapeDtypeStruct((3, PANEL, PANEL), F32),
            jax.ShapeDtypeStruct((4, 4, BLOCK, 2 * PANEL), F32),
            jax.ShapeDtypeStruct((2, PANEL, PANEL), F32),
        ],
        in_specs=[pl.BlockSpec(memory_space=pl.ANY)],
        out_specs=[
            pl.BlockSpec(memory_space=pltpu.VMEM),
            pl.BlockSpec(memory_space=pl.ANY),
            pl.BlockSpec(memory_space=pl.ANY),
        ],
        scratch_shapes=[
            pltpu.VMEM((PANEL, PANEL), F32),
            pltpu.VMEM((PANEL, PANEL), F32),
            (dma, dma, dma, dma((3,)), dma((3,)), dma((3, 3, 3)), dma((3, 3, 3)), dma((3,)), dma((3,)),
             dma((4,)), dma((2,)), dma((2,)), dma((2,)), dma((16,)), dma((16,))),
        ],
        compiler_params=pltpu.CompilerParams(has_side_effects=True, vmem_limit_bytes=24 * 2**20),
        name="gather",
    )(layer)


def product(a, b, precision=lax.Precision.HIGH):
    return lax.dot_general(a, b, (((1,), (1,)), ((), ())), precision=precision, preferred_element_type=F32)


def solved(a0, a1, v, precision):
    c0 = product(a0, v[:PANEL, :PANEL], precision)
    c1 = product(a0, v[PANEL:, :PANEL], precision) + product(a1, v[PANEL:, PANEL:], precision)
    return c0, c1


def per_device(layers):
    r = lax.axis_index("row")
    z = lax.axis_index("col")
    d = lax.axis_index("depth")
    layer = layers[0]
    lead, column_rows, own_rows = gather_panels(layer)
    v = inverse_cholesky(lead)
    g = column_rows.reshape(4 * PANEL, 2 * PANEL)
    swap = [(0, 1), (1, 0)]

    c0, c1 = solved(own_rows[0], own_rows[1], v, HI)
    block = r + 16 * d
    c1 = jnp.where(block >= 1, c1, 0.0)
    own = jnp.concatenate([c0, c1], axis=1)
    peer = lax.ppermute(own, "depth", swap)
    both = jnp.where(d == 0, jnp.stack([own, peer]), jnp.stack([peer, own])).reshape(2 * PANEL, 2 * PANEL)
    half = PANEL // 2
    factor = jnp.stack(
        [jnp.where(d == 0, both[:, p * PANEL : p * PANEL + half], both[:, p * PANEL + half : (p + 1) * PANEL]) for p in range(2)]
    )

    row_block = jnp.arange(2 * PANEL, dtype=jnp.int32) // PANEL * 16 + r
    panel = jnp.arange(2 * PANEL, dtype=jnp.int32) // PANEL
    left = jnp.where(row_block[:, None] > panel[None, :], both, 0.0)
    k0, k1 = solved(g[:, :PANEL], g[:, PANEL:], v, lax.Precision.HIGH)
    col_block = (jnp.arange(4 * PANEL, dtype=jnp.int32) // PANEL + 4 * d) * 4 + z
    right = jnp.where(col_block[:, None] > panel[None, :], jnp.concatenate([k0, k1], axis=1), 0.0)

    width = 4 * PANEL
    near = lax.dynamic_slice_in_dim(layer, d * width, width, 1)
    rows_peer = (1 - d) * PANEL
    far_peer = lax.dynamic_slice(layer, (rows_peer, (1 - d) * width), (PANEL, width))
    far_mine = lax.dynamic_slice(layer, (d * PANEL, (1 - d) * width), (PANEL, width))
    raw = lax.ppermute(far_peer, "depth", swap)
    updated = near - product(left, right)
    sent = lax.dynamic_slice_in_dim(updated, rows_peer, PANEL, 0)
    kept = lax.dynamic_slice_in_dim(updated, d * PANEL, PANEL, 0)
    got = lax.ppermute(sent, "depth", swap)
    here = kept + raw
    there = far_mine + got
    schur = jnp.where(d == 0, jnp.concatenate([here, there], axis=1), jnp.concatenate([there, here], axis=1))
    return factor, schur


def solution(mesh):
    return jax.shard_map(
        per_device,
        mesh=mesh,
        in_specs=(P("depth", "row", "col"),),
        out_specs=(P(None, "row", "depth"), P(("row", "depth"), "col")),
        check_vma=False,
    )
```

```python
import jax
import jax.numpy as jnp
from jax import lax
from jax.experimental import pallas as pl
from jax.experimental.pallas import tpu as pltpu
from jax.sharding import PartitionSpec as P

PANEL = 512
BLOCK = 128
HI = lax.Precision.HIGHEST
MESH = pl.DeviceIdType.MESH
F32 = jnp.float32
BF16 = jnp.bfloat16


def inverse_factor(x):
    n = x.shape[0]
    lane8 = lax.broadcasted_iota(jnp.int32, (8, n), 1)
    sub8 = lax.broadcasted_iota(jnp.int32, (8, n), 0)
    out = []
    for k in range(n // 8):
        lo = 8 * k
        head, rest = x[:8], x[8:]
        ck = [jnp.broadcast_to(head[:, lo + j : lo + j + 1], (8, n)) for j in range(8)]
        inblk = (lane8 >= lo) & (lane8 < lo + 8)
        head = jnp.where(inblk, jnp.where(lane8 - lo == sub8, 1.0, 0.0), head)
        more = rest.shape[0] > 0
        if more:
            cr = [jnp.broadcast_to(rest[:, lo + j : lo + j + 1], rest.shape) for j in range(8)]
            lane = lax.broadcasted_iota(jnp.int32, rest.shape, 1)
            rest = jnp.where((lane >= lo) & (lane < lo + 8), 0.0, rest)
        pivots = ck[0]
        for j in range(8):
            if j:
                pivots = jnp.where(sub8 == j, ck[j], pivots)
            inv = 1.0 / ck[j][j : j + 1, :]
            mk = jnp.where(sub8 > j, ck[j], 0.0) * inv
            if more:
                mr = cr[j] * inv
            for t in range(j + 1, 8):
                row = ck[t][j : j + 1, :]
                ck[t] = ck[t] - mk * row
                if more:
                    cr[t] = cr[t] - mr * row
            row = head[j : j + 1, :]
            head = head - mk * row
            if more:
                rest = rest - mr * row
        out.append(jnp.where(lane8 <= sub8 + lo, head, 0.0) * lax.rsqrt(pivots))
        x = rest
    return jnp.concatenate(out, axis=0)


def factor_steps(v_ref, urow, between):
    size = v_ref.shape[0]
    blocks = size // BLOCK

    def step(j, carry):
        between(j)
        off = pl.multiple_of(j * BLOCK, BLOCK)
        here = pl.ds(off, BLOCK)
        w = inverse_factor(v_ref[here, here])
        urow[...] = jnp.dot(w, v_ref[here, :], precision=HI, preferred_element_type=F32)
        urow[:, here] = w
        for i in range(1, blocks):

            @pl.when(i > j)
            def _():
                rows = pl.ds(i * BLOCK, BLOCK)
                v_ref[rows, here] = jnp.zeros((BLOCK, BLOCK), F32)
                v_ref[rows, :] -= lax.dot_general(
                    urow[:, rows],
                    urow[...],
                    (((0,), (0,)), ((), ())),
                    precision=HI,
                    preferred_element_type=F32,
                )

        lane = lax.broadcasted_iota(jnp.int32, (BLOCK, size), 1)
        v_ref[here, :] = jnp.where(lane < off + BLOCK, urow[...], 0.0)
        return carry

    lax.fori_loop(0, blocks, step, 0)


def product(a, b, precision):
    return lax.dot_general(a, b, (((1,), (1,)), ((), ())), precision=precision, preferred_element_type=F32)


def split(a):
    high = a.astype(BF16)
    return high, (a - high.astype(F32)).astype(BF16)


def three(ah, al, bh, bl):
    low = product(ah, bl, None) + product(al, bh, None)
    return product(ah, bh, None) + low


ORDERS = ((2, 1, 0), (0, 2, 1), (1, 0, 2))
LEADS = ((0, 0), (0, PANEL), (PANEL, PANEL))
SOURCES = ((0, 0, 0), (0, 0, 1), (1, 0, 1))


def panels_kernel(
    layer, rows_out, high_out, low_out, raw_out, got_out,
    v, urow, g_out, o_out, theirs, q, sent, vh, vl, peer_h, peer_l, sem,
):
    (swap_s, swap_r, half_s, dsc_s, dsc_r, dph_s, dph_r, dsw_s, dsw_r,
     sc_s, sc_r, own_s, own_r, ag_s, ag_r, raw_s, raw_r, got_s, got_r, row_s, row_r, near_s) = sem
    r = lax.axis_index("row")
    z = lax.axis_index("col")
    d = lax.axis_index("depth")
    x = lax.rem(r, 4)
    y = lax.div(r, 4)
    here = (x, y, z)

    def device(c, depth):
        return (c[1] * 4 + c[0], c[2], depth)

    def remote(src, dst, send, recv, target):
        return pltpu.make_async_remote_copy(
            src_ref=src, dst_ref=dst, send_sem=send, recv_sem=recv, device_id=target, device_id_type=MESH
        )

    def moved(axis, by):
        c = list(here)
        c[axis] = lax.rem(c[axis] + by, 4)
        return tuple(c)

    mine = pl.ds(pl.multiple_of(d * PANEL, PANEL), PANEL)
    other = pl.ds(pl.multiple_of((1 - d) * PANEL, PANEL), PANEL)
    cols = pl.ds(0, PANEL)
    swap = remote(layer.at[other, cols], theirs, swap_s, swap_r, device(here, 1 - d))
    swap.start()
    local = pltpu.make_async_copy(layer.at[mine, cols], q, half_s)
    local.start()
    local.wait()
    swap.wait()
    q[...] = q[...] + theirs[...]

    width = 4 * PANEL
    near = pl.ds(pl.multiple_of(d * width, width), width)
    far = pl.ds(pl.multiple_of((1 - d) * width, width), width)
    v[PANEL:, :PANEL] = jnp.zeros((PANEL, PANEL), F32)

    def lead(b, rows, columns):
        down, right = LEADS[b]
        return v.at[pl.ds(rows[0] + down, rows[1]), pl.ds(pl.multiple_of(columns + right, PANEL // 2), PANEL // 2)]

    half = PANEL // 2
    for b in range(3):
        sx, sy, sz = SOURCES[b]
        a1, a2, a3 = ORDERS[b]

        @pl.when((x == sx) & (y == sy) & (z == sz) & (d == 0))
        def _():
            def send(i, carry):
                c = [None] * 3
                piece = lax.div(i, 2)
                depth = lax.rem(i, 2)
                c[a1] = lax.rem(piece, 4)
                c[a2] = lax.rem(lax.div(piece, 4), 4)
                c[a3] = lax.div(piece, 16)
                first = pl.multiple_of(piece * 8, 8)
                rows = pl.ds(first, 8)
                part = pl.ds(pl.multiple_of(depth * half, half), half)
                target = lead(b, (first, 8), depth * half)
                own = (c[0] == sx) & (c[1] == sy) & (c[2] == sz) & (depth == 0)

                @pl.when(jnp.logical_not(own))
                def _():
                    remote(q.at[rows, part], target, dsc_s.at[b], dsc_r.at[b], device(c, depth)).start()

                @pl.when(own)
                def _():
                    pltpu.make_async_copy(q.at[rows, part], target, dsc_r.at[b]).start()

                return carry

            lax.fori_loop(0, 128, send, 0)

    for p in range(2):

        @pl.when(z == p)
        def _():
            for k in range(4):
                rows = pl.ds(k * BLOCK, BLOCK)
                target = g_out.at[y, k, :, pl.ds(p * PANEL, PANEL)]
                own = (x == p) & (x == k)

                @pl.when(jnp.logical_not(own))
                def _():
                    remote(q.at[rows, :], target, sc_s.at[k], sc_r.at[p], device((k, y, x), d)).start()

                @pl.when(own)
                def _():
                    pltpu.make_async_copy(q.at[rows, :], target, sc_r.at[p]).start()

    part = pl.ds(pl.multiple_of(d * half, half), half)

    def region(b, phase):
        a1, a2, a3 = ORDERS[b]
        c = here
        if phase == 0:
            return c[a3] * 128 + c[a2] * 32 + c[a1] * 8, 8
        if phase == 1:
            return c[a3] * 128 + c[a2] * 32, 32
        return c[a3] * 128, 128

    def phase_copy(b, phase, by):
        start, rows = region(b, phase)
        ref = lead(b, (pl.multiple_of(start, rows), rows), d * half)
        return remote(
            ref, ref, dph_s.at[b, phase, by - 1], dph_r.at[b, phase, by - 1], device(moved(ORDERS[b][phase], by), d)
        )

    def sized(ref, s):
        return pltpu.make_async_copy(ref, ref, s)

    for b in range(3):
        sized(urow.at[pl.ds(0, 8), pl.ds(0, half)], dsc_r.at[b]).wait()
        for by in (1, 2, 3):
            phase_copy(b, 0, by).start()
    for phase in (1, 2):
        for b in range(3):
            for by in (1, 2, 3):
                phase_copy(b, phase - 1, by).wait_recv()
            for by in (1, 2, 3):
                phase_copy(b, phase, by).start()
    for b in range(3):
        for by in (1, 2, 3):
            phase_copy(b, 2, by).wait_recv()

        ref = lead(b, (0, PANEL), d * half)
        remote(ref, ref, dsw_s.at[b], dsw_r.at[b], device(here, 1 - d)).start()

    def own_copy(p, to, slot):
        src = q
        return remote(src, o_out.at[p], own_s.at[slot], own_r.at[p], device((x, y, to), d))

    for p in range(2):

        @pl.when(z == p)
        def _():
            pltpu.make_async_copy(q, o_out.at[p], own_r.at[p]).start()
            own_copy(p, 1 - p, 0).start()
            own_copy(p, 3 - p, 1).start()

    for b in range(3):
        ref = lead(b, (0, PANEL), d * half)
        remote(ref, ref, dsw_s.at[b], dsw_r.at[b], device(here, 1 - d)).wait()
        for phase in range(3):
            for by in (1, 2, 3):
                phase_copy(b, phase, by).wait_send()
        sx, sy, sz = SOURCES[b]

        @pl.when((x == sx) & (y == sy) & (z == sz) & (d == 0))
        def _():
            sized(layer.at[pl.ds(0, 127 * 8), pl.ds(0, half)], dsc_s.at[b]).wait()

    def ag_ref(h, phase, c, piece):
        cx, cy = c
        part = pl.ds(h * PANEL, PANEL)
        if phase == 0:
            rows = {None: pl.ds(0, 128), 0: pl.ds(0, 64), 1: pl.ds(64, 64)}[piece]
            return g_out.at[cy, cx, rows, part]
        span = {None: pl.ds(0, 4), 0: pl.ds(0, 2), 1: pl.ds(2, 2)}[piece]
        if h == 0:
            return g_out.at[cy, span, :, part]
        return g_out.at[span, cx, :, part]

    def ag_copy(h, phase, stage, way):
        axis = (phase + h) % 2
        by = 1 if way == 0 else 3
        c = here if stage == 0 else moved(axis, 4 - by)
        ref = ag_ref(h, phase, (c[0], c[1]), None if stage == 0 else way)
        slot = ((h * 2 + phase) * 2 + stage) * 2 + way
        return remote(ref, ref, ag_s.at[slot], ag_r.at[slot], device(moved(axis, by), d))

    for h in range(2):
        sized(g_out.at[0, 0, :, pl.ds(0, PANEL)], sc_r.at[h]).wait()
        for way in range(2):
            ag_copy(h, 0, 0, way).start()
    remote(layer.at[other, far], raw_out, raw_s, raw_r, device(here, 1 - d)).start()
    pltpu.make_async_copy(layer.at[other, near], sent, near_s).start()

    def received(phase, stage):
        for h in range(2):
            for way in range(2):
                ag_copy(h, phase, stage, way).wait_recv()

    def started(phase, stage):
        for h in range(2):
            for way in range(2):
                ag_copy(h, phase, stage, way).start()

    def between(j):
        @pl.when(j == 1)
        def _():
            received(0, 0)
            started(0, 1)

        @pl.when(j == 2)
        def _():
            received(0, 1)
            started(1, 0)

        for p in range(2):

            @pl.when((j == 4) & (z == 3 - p))
            def _():
                sized(o_out.at[p], own_r.at[p]).wait()
                ref = o_out.at[p]
                remote(ref, ref, own_s.at[0], own_r.at[p], device((x, y, 2 + p), d)).start()

        @pl.when(j == 6)
        def _():
            received(1, 0)
            started(1, 1)

    factor_steps(v, urow, between)
    vh[...] = v[...].astype(BF16)
    vl[...] = (v[...] - vh[...].astype(F32)).astype(BF16)

    for p in range(2):

        @pl.when(z != 3 - p)
        def _():
            sized(o_out.at[p], own_r.at[p]).wait()

    c0 = product(o_out[0], v[:PANEL, :PANEL], HI)
    c1 = product(o_out[0], v[PANEL:, :PANEL], HI) + product(o_out[1], v[PANEL:, PANEL:], HI)
    rows_out[mine, :PANEL] = c0
    rows_out[mine, PANEL:] = jnp.where(r + 16 * d >= 1, c1, 0.0)
    rows = remote(rows_out.at[mine, :], rows_out.at[mine, :], row_s, row_r, device(here, 1 - d))
    rows.start()

    received(1, 1)

    def solve(k, carry):
        a = g_out[k].reshape(PANEL, 2 * PANEL)
        ah, al = split(a)
        here = pl.ds(pl.multiple_of(k * PANEL, PANEL), PANEL)
        block = (k + 4 * d) * 4 + z
        for p in range(2):
            depth = slice(0, (p + 1) * PANEL)
            out = slice(p * PANEL, (p + 1) * PANEL)
            c = three(ah[:, depth], al[:, depth], vh[out, depth], vl[out, depth])
            ch, cl = split(jnp.where(block > p, c, 0.0))
            high_out[here, out] = ch
            low_out[here, out] = cl
        return carry

    lax.fori_loop(0, 4, solve, 0)

    rows.wait()
    for p in range(2):
        out = slice(p * PANEL, (p + 1) * PANEL)
        ch, cl = split(jnp.where(r + 16 * (1 - d) > p, rows_out[other, out], 0.0))
        peer_h[:, out] = ch
        peer_l[:, out] = cl
    pltpu.make_async_copy(layer.at[other, near], sent, near_s).wait()

    def got_copy(k):
        tile = pl.ds(pl.multiple_of(k * PANEL, PANEL), PANEL)
        return remote(sent.at[:, tile], got_out.at[:, tile], got_s.at[k], got_r.at[k], device(here, 1 - d))

    def update(k, carry):
        tile = pl.ds(pl.multiple_of(k * PANEL, PANEL), PANEL)
        sent[:, tile] -= three(peer_h[...], peer_l[...], high_out[tile, :], low_out[tile, :])
        got_copy(k).start()
        return carry

    lax.fori_loop(0, 4, update, 0)
    for k in range(4):
        got_copy(k).wait()
    remote(layer.at[other, far], raw_out, raw_s, raw_r, device(here, 1 - d)).wait()

    for h in range(2):
        for phase in range(2):
            for stage in range(2):
                for way in range(2):
                    ag_copy(h, phase, stage, way).wait_send()

    @pl.when(z < 2)
    def _():
        sized(q, own_s.at[0]).wait()
        sized(q, own_s.at[1]).wait()

    @pl.when(z >= 2)
    def _():
        sized(q, own_s.at[0]).wait()

    for k in range(4):

        @pl.when((z < 2) & jnp.logical_not((x == z) & (x == k)))
        def _():
            sized(q.at[pl.ds(0, BLOCK), :], sc_s.at[k]).wait()


def panels(layer):
    dma = pltpu.SemaphoreType.DMA
    width = 4 * PANEL
    size = 2 * PANEL
    vmem = pl.BlockSpec(memory_space=pltpu.VMEM)
    hbm = pl.BlockSpec(memory_space=pltpu.HBM)
    return pl.pallas_call(
        panels_kernel,
        out_shape=[
            jax.ShapeDtypeStruct((size, size), F32),
            jax.ShapeDtypeStruct((width, size), BF16),
            jax.ShapeDtypeStruct((width, size), BF16),
            jax.ShapeDtypeStruct((PANEL, width), F32),
            jax.ShapeDtypeStruct((PANEL, width), F32),
        ],
        in_specs=[hbm],
        out_specs=[vmem, vmem, vmem, hbm, hbm],
        scratch_shapes=[
            pltpu.VMEM((size, size), F32),
            pltpu.VMEM((BLOCK, size), F32),
            pltpu.VMEM((4, 4, BLOCK, size), F32),
            pltpu.VMEM((2, PANEL, PANEL), F32),
            pltpu.VMEM((PANEL, PANEL), F32),
            pltpu.VMEM((PANEL, PANEL), F32),
            pltpu.VMEM((PANEL, width), F32),
            pltpu.VMEM((size, size), BF16),
            pltpu.VMEM((size, size), BF16),
            pltpu.VMEM((PANEL, size), BF16),
            pltpu.VMEM((PANEL, size), BF16),
            (dma, dma, dma, dma((3,)), dma((3,)), dma((3, 3, 3)), dma((3, 3, 3)), dma((3,)), dma((3,)),
             dma((4,)), dma((2,)), dma((2,)), dma((2,)), dma((16,)), dma((16,)),
             dma, dma, dma((4,)), dma((4,)), dma, dma, dma),
        ],
        compiler_params=pltpu.CompilerParams(has_side_effects=True, vmem_limit_bytes=60 * 2**20),
        name="panels",
    )(layer)


def finish_kernel(info, layer, raw, got, rows_own, rows_all, high, low, schur, factor, own_h, own_l):
    t = pl.program_id(0)
    d = info[0]
    r = info[1]

    @pl.when(t == 0)
    def _():
        for p in range(2):
            out = slice(p * PANEL, (p + 1) * PANEL)
            ch, cl = split(jnp.where(r + 16 * d > p, rows_own[:, out], 0.0))
            own_h[:, out] = ch
            own_l[:, out] = cl

    @pl.when(t < 4)
    def _():
        schur[...] = layer[...] + raw[...] - three(own_h[...], own_l[...], high[...], low[...])

    @pl.when(t >= 4)
    def _():
        schur[...] = layer[...] + got[...]

    half = PANEL // 2
    for p in range(2):
        first = rows_all[:, p * PANEL : p * PANEL + half]
        factor[p] = jnp.where(d == 0, first, rows_all[:, p * PANEL + half : (p + 1) * PANEL])


def finish(info, layer, raw, got, rows, high, low):
    width = 4 * PANEL
    size = 2 * PANEL

    def place(t, info):
        d = info[0]
        return jnp.where(t < 4, 4 * d + t, 4 * (1 - d) + t - 4)

    def tile(index):
        return pl.BlockSpec((PANEL, PANEL), index)

    return pl.pallas_call(
        finish_kernel,
        out_shape=[
            jax.ShapeDtypeStruct((PANEL, 2 * width), F32),
            jax.ShapeDtypeStruct((2, size, PANEL // 2), F32),
        ],
        grid_spec=pltpu.PrefetchScalarGridSpec(
            num_scalar_prefetch=1,
            grid=(8,),
            in_specs=[
                tile(lambda t, info: (info[0], place(t, info))),
                tile(lambda t, info: (0, jnp.minimum(t, 3))),
                tile(lambda t, info: (0, jnp.maximum(t - 4, 0))),
                pl.BlockSpec((PANEL, size), lambda t, info: (info[0], 0)),
                pl.BlockSpec((BLOCK, size), lambda t, info: (t, 0)),
                pl.BlockSpec((PANEL, size), lambda t, info: (jnp.minimum(t, 3), 0)),
                pl.BlockSpec((PANEL, size), lambda t, info: (jnp.minimum(t, 3), 0)),
            ],
            out_specs=[
                tile(lambda t, info: (0, place(t, info))),
                pl.BlockSpec((2, BLOCK, PANEL // 2), lambda t, info: (0, t, 0)),
            ],
            scratch_shapes=[pltpu.VMEM((PANEL, size), BF16), pltpu.VMEM((PANEL, size), BF16)],
        ),
        compiler_params=pltpu.CompilerParams(vmem_limit_bytes=40 * 2**20),
        name="finish",
    )(info, layer, raw, got, rows, rows, high, low)


def per_device(layers):
    layer = layers[0]
    info = jnp.stack([lax.axis_index("depth"), lax.axis_index("row")]).astype(jnp.int32)
    rows, high, low, raw, got = panels(layer)
    schur, factor = finish(info, layer, raw, got, rows, high, low)
    return factor, schur


def solution(mesh):
    return jax.shard_map(
        per_device,
        mesh=mesh,
        in_specs=(P("depth", "row", "col"),),
        out_specs=(P(None, "row", "depth"), P(("row", "depth"), "col")),
        check_vma=False,
    )
```

```python
import jax
import jax.numpy as jnp
from jax import lax
from jax.experimental import pallas as pl
from jax.experimental.pallas import tpu as pltpu
from jax.sharding import PartitionSpec as P

PANEL = 512
BLOCK = 128
HI = lax.Precision.HIGHEST
MESH = pl.DeviceIdType.MESH
F32 = jnp.float32
BF16 = jnp.bfloat16


def inverse_factor(x):
    n = x.shape[0]
    lane8 = lax.broadcasted_iota(jnp.int32, (8, n), 1)
    sub8 = lax.broadcasted_iota(jnp.int32, (8, n), 0)
    out = []
    for k in range(n // 8):
        lo = 8 * k
        head, rest = x[:8], x[8:]
        ck = [jnp.broadcast_to(head[:, lo + j : lo + j + 1], (8, n)) for j in range(8)]
        inblk = (lane8 >= lo) & (lane8 < lo + 8)
        head = jnp.where(inblk, jnp.where(lane8 - lo == sub8, 1.0, 0.0), head)
        more = rest.shape[0] > 0
        if more:
            cr = [jnp.broadcast_to(rest[:, lo + j : lo + j + 1], rest.shape) for j in range(8)]
            lane = lax.broadcasted_iota(jnp.int32, rest.shape, 1)
            rest = jnp.where((lane >= lo) & (lane < lo + 8), 0.0, rest)
        pivots = ck[0]
        for j in range(8):
            if j:
                pivots = jnp.where(sub8 == j, ck[j], pivots)
            inv = 1.0 / ck[j][j : j + 1, :]
            mk = jnp.where(sub8 > j, ck[j], 0.0) * inv
            if more:
                mr = cr[j] * inv
            for t in range(j + 1, 8):
                row = ck[t][j : j + 1, :]
                ck[t] = ck[t] - mk * row
                if more:
                    cr[t] = cr[t] - mr * row
            row = head[j : j + 1, :]
            head = head - mk * row
            if more:
                rest = rest - mr * row
        out.append(jnp.where(lane8 <= sub8 + lo, head, 0.0) * lax.rsqrt(pivots))
        x = rest
    return jnp.concatenate(out, axis=0)


def factor_steps(v_ref, urow, between):
    size = v_ref.shape[0]
    blocks = size // BLOCK

    def step(j, carry):
        between(j)
        off = pl.multiple_of(j * BLOCK, BLOCK)
        here = pl.ds(off, BLOCK)
        w = inverse_factor(v_ref[here, here])
        urow[...] = jnp.dot(w, v_ref[here, :], precision=HI, preferred_element_type=F32)
        urow[:, here] = w
        for i in range(1, blocks):

            @pl.when(i > j)
            def _():
                rows = pl.ds(i * BLOCK, BLOCK)
                v_ref[rows, here] = jnp.zeros((BLOCK, BLOCK), F32)
                v_ref[rows, :] -= lax.dot_general(
                    urow[:, rows],
                    urow[...],
                    (((0,), (0,)), ((), ())),
                    precision=HI,
                    preferred_element_type=F32,
                )

        lane = lax.broadcasted_iota(jnp.int32, (BLOCK, size), 1)
        v_ref[here, :] = jnp.where(lane < off + BLOCK, urow[...], 0.0)
        return carry

    lax.fori_loop(0, blocks, step, 0)


def product(a, b, precision, contract=1):
    return lax.dot_general(a, b, (((1,), (contract,)), ((), ())), precision=precision, preferred_element_type=F32)


def split(a):
    high = a.astype(BF16)
    return high, (a - high.astype(F32)).astype(BF16)


def three(ah, al, bh, bl, contract=1):
    low = product(ah, bl, None, contract) + product(al, bh, None, contract)
    return product(ah, bh, None, contract) + low


ORDERS = ((2, 1, 0), (0, 2, 1), (1, 0, 2))
LEADS = ((0, 0), (0, PANEL), (PANEL, PANEL))
SOURCES = ((0, 0, 0), (0, 0, 1), (1, 0, 1))


def panels_kernel(
    layer, rows_hbm, high_hbm, low_hbm, raw_out, got_out,
    rows_out, high_out, low_out, v, urow, g_out, o_out, theirs, q, sent, vh, vl, peer_h, peer_l, sem,
):
    (swap_s, swap_r, half_s, first_s, first_r, second_s, second_r, dph_s, dph_r, dsw_s, dsw_r,
     sc_s, sc_r, own_s, own_r, ag_s, ag_r, raw_s, raw_r, got_s, got_r, row_s, row_r, near_s, put) = sem
    r = lax.axis_index("row")
    z = lax.axis_index("col")
    d = lax.axis_index("depth")
    x = lax.rem(r, 4)
    y = lax.div(r, 4)
    here = (x, y, z)

    def device(c, depth):
        return (c[1] * 4 + c[0], c[2], depth)

    def remote(src, dst, send, recv, target):
        return pltpu.make_async_remote_copy(
            src_ref=src, dst_ref=dst, send_sem=send, recv_sem=recv, device_id=target, device_id_type=MESH
        )

    def moved(axis, by):
        c = list(here)
        c[axis] = lax.rem(c[axis] + by, 4)
        return tuple(c)

    mine = pl.ds(pl.multiple_of(d * PANEL, PANEL), PANEL)
    other = pl.ds(pl.multiple_of((1 - d) * PANEL, PANEL), PANEL)
    cols = pl.ds(0, PANEL)
    swap = remote(layer.at[other, cols], theirs, swap_s, swap_r, device(here, 1 - d))
    swap.start()
    local = pltpu.make_async_copy(layer.at[mine, cols], q, half_s)
    local.start()
    local.wait()
    swap.wait()
    q[...] = q[...] + theirs[...]

    width = 4 * PANEL
    near = pl.ds(pl.multiple_of(d * width, width), width)
    far = pl.ds(pl.multiple_of((1 - d) * width, width), width)
    v[PANEL:, :PANEL] = jnp.zeros((PANEL, PANEL), F32)

    def lead(b, rows, columns):
        down, right = LEADS[b]
        return v.at[pl.ds(rows[0] + down, rows[1]), pl.ds(pl.multiple_of(columns + right, PANEL // 2), PANEL // 2)]

    half = PANEL // 2

    def at(b, axes):
        same = here[axes[0]] == SOURCES[b][axes[0]]
        for axis in axes[1:]:
            same = same & (here[axis] == SOURCES[b][axis])
        return same

    def sized(ref, s):
        return pltpu.make_async_copy(ref, ref, s)

    def piece(b, stage, t=None):
        a1, a2, a3 = ORDERS[b]
        if stage == 0:
            return lead(b, (pl.multiple_of(here[a3] * 128, 128), 128), d * half)
        t = here[a2] if t is None else t
        return lead(b, (pl.multiple_of(here[a3] * 128 + t * 32, 32), 32), d * half)

    def cut(b, t, depth):
        c = list(here)
        c[ORDERS[b][2]] = t
        src = q.at[pl.ds(128 * t, 128), pl.ds(depth * half, half)]
        down, right = LEADS[b]
        dst = v.at[pl.ds(down + 128 * t, 128), pl.ds(right + depth * half, half)]
        if t == SOURCES[b][ORDERS[b][2]] and depth == 0:
            return pltpu.make_async_copy(src, dst, first_r.at[b])
        return remote(src, dst, first_s.at[b, t, depth], first_r.at[b], device(c, depth))

    def cuts(b, act):
        @pl.when(at(b, (0, 1, 2)) & (d == 0))
        def _():
            for t in range(4):
                for depth in range(2):
                    if act == "start":
                        cut(b, t, depth).start()
                    elif not (t == SOURCES[b][ORDERS[b][2]] and depth == 0):
                        cut(b, t, depth).wait_send()

    def second(b, t):
        c = list(here)
        c[ORDERS[b][1]] = t
        ref = piece(b, 1, t)
        return remote(ref, ref, second_s.at[b, t], second_r.at[b], device(c, d))

    def along(b, stage, by):
        axis = ORDERS[b][stage]
        ref = piece(b, 0 if stage == 2 else 1)
        return remote(ref, ref, dph_s.at[b, stage, by - 1], dph_r.at[b, stage, by - 1], device(moved(axis, by), d))

    def copied(b):
        axis = ORDERS[b][0]
        for by in (1, 2, 3):

            @pl.when(lax.rem(here[axis] - by + 4, 4) == SOURCES[b][axis])
            def _():
                along(b, 0, by).wait_recv()

    def wanted(b, act):
        a1, a2, a3 = ORDERS[b]
        for by in (1, 2, 3):

            @pl.when(jnp.logical_not(at(b, (a1,)) & (lax.rem(here[a2] + by, 4) == SOURCES[b][a2])))
            def _():
                if act == "start":
                    along(b, 1, by).start()
                else:
                    along(b, 1, by).wait_send()

    for b in range(3):
        cuts(b, "start")
    for b in range(3):
        a1, a2, a3 = ORDERS[b]

        @pl.when(at(b, (a1, a2)))
        def _():
            sized(piece(b, 0), first_r.at[b]).wait()
            for t in range(4):
                if t != SOURCES[b][a2]:
                    second(b, t).start()

    for b in range(3):
        a1, a2, a3 = ORDERS[b]

        @pl.when(at(b, (a1,)))
        def _():
            @pl.when(jnp.logical_not(at(b, (a2,))))
            def _():
                sized(piece(b, 1), second_r.at[b]).wait()

            for by in (1, 2, 3):
                along(b, 0, by).start()

    for p in range(2):

        @pl.when(z == p)
        def _():
            for k in range(4):
                rows = pl.ds(k * BLOCK, BLOCK)
                target = g_out.at[y, k, :, pl.ds(p * PANEL, PANEL)]
                own = (x == p) & (x == k)

                @pl.when(jnp.logical_not(own))
                def _():
                    remote(q.at[rows, :], target, sc_s.at[k], sc_r.at[p], device((k, y, x), d)).start()

                @pl.when(own)
                def _():
                    pltpu.make_async_copy(q.at[rows, :], target, sc_r.at[p]).start()

    for b in range(3):
        copied(b)
        wanted(b, "start")
    for b in range(3):
        @pl.when(jnp.logical_not(at(b, ORDERS[b][:2])))
        def _():
            for by in (1, 2, 3):
                along(b, 1, by).wait_recv()

        for by in (1, 2, 3):
            along(b, 2, by).start()
    for b in range(3):
        for by in (1, 2, 3):
            along(b, 2, by).wait_recv()
        ref = lead(b, (0, PANEL), d * half)
        remote(ref, ref, dsw_s.at[b], dsw_r.at[b], device(here, 1 - d)).start()

    def own_copy(p, to, slot):
        src = q
        return remote(src, o_out.at[p], own_s.at[slot], own_r.at[p], device((x, y, to), d))

    for p in range(2):

        @pl.when(z == p)
        def _():
            pltpu.make_async_copy(q, o_out.at[p], own_r.at[p]).start()
            own_copy(p, 1 - p, 0).start()
            own_copy(p, 3 - p, 1).start()

    for b in range(3):
        ref = lead(b, (0, PANEL), d * half)
        remote(ref, ref, dsw_s.at[b], dsw_r.at[b], device(here, 1 - d)).wait()
        a1, a2, a3 = ORDERS[b]
        wanted(b, "wait")
        for by in (1, 2, 3):
            along(b, 2, by).wait_send()
        cuts(b, "wait")

        @pl.when(at(b, (a1, a2)))
        def _():
            for t in range(4):
                if t != SOURCES[b][a2]:
                    second(b, t).wait_send()

        @pl.when(at(b, (a1,)))
        def _():
            for by in (1, 2, 3):
                along(b, 0, by).wait_send()

    def ag_ref(h, phase, c, piece):
        cx, cy = c
        part = pl.ds(h * PANEL, PANEL)
        if phase == 0:
            rows = {None: pl.ds(0, 128), 0: pl.ds(0, 64), 1: pl.ds(64, 64)}[piece]
            return g_out.at[cy, cx, rows, part]
        span = {None: pl.ds(0, 4), 0: pl.ds(0, 2), 1: pl.ds(2, 2)}[piece]
        if h == 0:
            return g_out.at[cy, span, :, part]
        return g_out.at[span, cx, :, part]

    def ag_copy(h, phase, stage, way):
        axis = (phase + h) % 2
        by = 1 if way == 0 else 3
        c = here if stage == 0 else moved(axis, 4 - by)
        ref = ag_ref(h, phase, (c[0], c[1]), None if stage == 0 else way)
        slot = ((h * 2 + phase) * 2 + stage) * 2 + way
        return remote(ref, ref, ag_s.at[slot], ag_r.at[slot], device(moved(axis, by), d))

    for h in range(2):
        sized(g_out.at[0, 0, :, pl.ds(0, PANEL)], sc_r.at[h]).wait()
        for way in range(2):
            ag_copy(h, 0, 0, way).start()
    remote(layer.at[other, far], raw_out, raw_s, raw_r, device(here, 1 - d)).start()
    pltpu.make_async_copy(layer.at[other, near], sent, near_s).start()

    def received(phase, stage):
        for h in range(2):
            for way in range(2):
                ag_copy(h, phase, stage, way).wait_recv()

    def started(phase, stage):
        for h in range(2):
            for way in range(2):
                ag_copy(h, phase, stage, way).start()

    def between(j):
        @pl.when(j == 1)
        def _():
            received(0, 0)
            started(0, 1)

        @pl.when(j == 2)
        def _():
            received(0, 1)
            started(1, 0)

        for p in range(2):

            @pl.when((j == 4) & (z == 3 - p))
            def _():
                sized(o_out.at[p], own_r.at[p]).wait()
                ref = o_out.at[p]
                remote(ref, ref, own_s.at[0], own_r.at[p], device((x, y, 2 + p), d)).start()

        @pl.when(j == 6)
        def _():
            received(1, 0)
            started(1, 1)

    factor_steps(v, urow, between)
    for k in range(4):
        part = slice(k * 256, (k + 1) * 256)
        th, tl = split(v[part, :].T)
        vh[:, part] = th
        vl[:, part] = tl

    for p in range(2):

        @pl.when(z != 3 - p)
        def _():
            sized(o_out.at[p], own_r.at[p]).wait()

    rows_out[mine, :PANEL] = product(o_out[0], v[:PANEL, :PANEL], HI)
    c1 = product(o_out[0], v[PANEL:, :PANEL], HI) + product(o_out[1], v[PANEL:, PANEL:], HI)
    rows_out[mine, PANEL:] = jnp.where(r + 16 * d >= 1, c1, 0.0)
    rows = remote(rows_out.at[mine, :], rows_out.at[mine, :], row_s, row_r, device(here, 1 - d))
    rows.start()

    received(1, 1)

    def solve(k, carry):
        a = g_out[k].reshape(PANEL, 2 * PANEL)
        ah, al = split(a)
        here = pl.ds(pl.multiple_of(k * PANEL, PANEL), PANEL)
        block = (k + 4 * d) * 4 + z
        for p in range(2):
            depth = slice(0, (p + 1) * PANEL)
            out = slice(p * PANEL, (p + 1) * PANEL)
            c = three(ah[:, depth], al[:, depth], vh[depth, out], vl[depth, out], 0)
            ch, cl = split(jnp.where(block > p, c, 0.0))
            high_out[here, out] = ch
            low_out[here, out] = cl
        return carry

    def put_copies(k):
        here = pl.ds(pl.multiple_of(k * PANEL, PANEL), PANEL)
        return (
            pltpu.make_async_copy(high_out.at[here, :], high_hbm.at[here, :], put.at[k]),
            pltpu.make_async_copy(low_out.at[here, :], low_hbm.at[here, :], put.at[4 + k]),
        )

    lax.fori_loop(0, 4, solve, 0)

    rows.wait()
    put_rows = pltpu.make_async_copy(rows_out, rows_hbm, put.at[8])
    put_rows.start()
    for k in range(4):
        for copy in put_copies(k):
            copy.start()
    for p in range(2):
        out = slice(p * PANEL, (p + 1) * PANEL)
        ch, cl = split(jnp.where(r + 16 * (1 - d) > p, rows_out[other, out], 0.0))
        peer_h[:, out] = ch
        peer_l[:, out] = cl
    pltpu.make_async_copy(layer.at[other, near], sent, near_s).wait()

    def got_copy(k):
        tile = pl.ds(pl.multiple_of(k * PANEL, PANEL), PANEL)
        return remote(sent.at[:, tile], got_out.at[:, tile], got_s.at[k], got_r.at[k], device(here, 1 - d))

    def update(k, carry):
        tile = pl.ds(pl.multiple_of(k * PANEL, PANEL), PANEL)
        sent[:, tile] -= three(peer_h[...], peer_l[...], high_out[tile, :], low_out[tile, :])
        got_copy(k).start()
        return carry

    lax.fori_loop(0, 4, update, 0)
    for k in range(4):
        got_copy(k).wait()
        for copy in put_copies(k):
            copy.wait()
    put_rows.wait()
    remote(layer.at[other, far], raw_out, raw_s, raw_r, device(here, 1 - d)).wait()

    for h in range(2):
        for phase in range(2):
            for stage in range(2):
                for way in range(2):
                    ag_copy(h, phase, stage, way).wait_send()

    @pl.when(z < 2)
    def _():
        sized(q, own_s.at[0]).wait()
        sized(q, own_s.at[1]).wait()

    @pl.when(z >= 2)
    def _():
        sized(q, own_s.at[0]).wait()

    for k in range(4):

        @pl.when((z < 2) & jnp.logical_not((x == z) & (x == k)))
        def _():
            sized(q.at[pl.ds(0, BLOCK), :], sc_s.at[k]).wait()


def panels(layer):
    dma = pltpu.SemaphoreType.DMA
    width = 4 * PANEL
    size = 2 * PANEL
    hbm = pl.BlockSpec(memory_space=pltpu.HBM)
    return pl.pallas_call(
        panels_kernel,
        out_shape=[
            jax.ShapeDtypeStruct((size, size), F32),
            jax.ShapeDtypeStruct((width, size), BF16),
            jax.ShapeDtypeStruct((width, size), BF16),
            jax.ShapeDtypeStruct((PANEL, width), F32),
            jax.ShapeDtypeStruct((PANEL, width), F32),
        ],
        in_specs=[hbm],
        out_specs=[hbm] * 5,
        scratch_shapes=[
            pltpu.VMEM((size, size), F32),
            pltpu.VMEM((width, size), BF16),
            pltpu.VMEM((width, size), BF16),
            pltpu.VMEM((size, size), F32),
            pltpu.VMEM((BLOCK, size), F32),
            pltpu.VMEM((4, 4, BLOCK, size), F32),
            pltpu.VMEM((2, PANEL, PANEL), F32),
            pltpu.VMEM((PANEL, PANEL), F32),
            pltpu.VMEM((PANEL, PANEL), F32),
            pltpu.VMEM((PANEL, width), F32),
            pltpu.VMEM((size, size), BF16),
            pltpu.VMEM((size, size), BF16),
            pltpu.VMEM((PANEL, size), BF16),
            pltpu.VMEM((PANEL, size), BF16),
            (dma, dma, dma, dma((3, 4, 2)), dma((3,)), dma((3, 4)), dma((3,)), dma((3, 3, 3)), dma((3, 3, 3)), dma((3,)), dma((3,)),
             dma((4,)), dma((2,)), dma((2,)), dma((2,)), dma((16,)), dma((16,)),
             dma, dma, dma((4,)), dma((4,)), dma, dma, dma, dma((9,))),
        ],
        compiler_params=pltpu.CompilerParams(has_side_effects=True, vmem_limit_bytes=60 * 2**20),
        name="panels",
    )(layer)


def finish_kernel(info, layer, raw, got, rows_own, first, second, high, low, schur, factor, own_h, own_l):
    t = pl.program_id(0)
    d = info[0]
    r = info[1]

    @pl.when(t == 0)
    def _():
        for p in range(2):
            out = slice(p * PANEL, (p + 1) * PANEL)
            ch, cl = split(jnp.where(r + 16 * d > p, rows_own[:, out], 0.0))
            own_h[:, out] = ch
            own_l[:, out] = cl

    @pl.when(t < 4)
    def _():
        schur[...] = layer[...] + raw[...] - three(own_h[...], own_l[...], high[...], low[...])

    @pl.when(t >= 4)
    def _():
        schur[...] = layer[...] + got[...]

    factor[0] = first[...]
    factor[1] = second[...]


def finish(info, layer, raw, got, rows, high, low):
    width = 4 * PANEL
    size = 2 * PANEL

    def place(t, info):
        d = info[0]
        return jnp.where(t < 4, 4 * d + t, 4 * (1 - d) + t - 4)

    def tile(index):
        return pl.BlockSpec((PANEL, PANEL), index)

    return pl.pallas_call(
        finish_kernel,
        out_shape=[
            jax.ShapeDtypeStruct((PANEL, 2 * width), F32),
            jax.ShapeDtypeStruct((2, size, PANEL // 2), F32),
        ],
        grid_spec=pltpu.PrefetchScalarGridSpec(
            num_scalar_prefetch=1,
            grid=(8,),
            in_specs=[
                tile(lambda t, info: (info[0], place(t, info))),
                tile(lambda t, info: (0, jnp.minimum(t, 3))),
                tile(lambda t, info: (0, jnp.maximum(t - 4, 0))),
                pl.BlockSpec((PANEL, size), lambda t, info: (info[0], 0)),
                pl.BlockSpec((BLOCK, PANEL // 2), lambda t, info: (t, info[0])),
                pl.BlockSpec((BLOCK, PANEL // 2), lambda t, info: (t, 2 + info[0])),
                pl.BlockSpec((PANEL, size), lambda t, info: (jnp.minimum(t, 3), 0)),
                pl.BlockSpec((PANEL, size), lambda t, info: (jnp.minimum(t, 3), 0)),
            ],
            out_specs=[
                tile(lambda t, info: (0, place(t, info))),
                pl.BlockSpec((2, BLOCK, PANEL // 2), lambda t, info: (0, t, 0)),
            ],
            scratch_shapes=[pltpu.VMEM((PANEL, size), BF16), pltpu.VMEM((PANEL, size), BF16)],
        ),
        compiler_params=pltpu.CompilerParams(vmem_limit_bytes=60 * 2**20),
        name="finish",
    )(info, layer, raw, got, rows, rows, rows, high, low)


def per_device(layers):
    layer = layers[0]
    info = jnp.stack([lax.axis_index("depth"), lax.axis_index("row")]).astype(jnp.int32)
    rows, high, low, raw, got = panels(layer)
    schur, factor = finish(info, layer, raw, got, rows, high, low)
    return factor, schur


def solution(mesh):
    return jax.shard_map(
        per_device,
        mesh=mesh,
        in_specs=(P("depth", "row", "col"),),
        out_specs=(P(None, "row", "depth"), P(("row", "depth"), "col")),
        check_vma=False,
    )
```
